32 devices in a mesh: sub: 4 (over x, core), lat: 2 (over y), lon: 4 (over z).
Axes of the slice: x: 2, y: 2, z: 4, core: 2. Of those that a mesh axis runs over, the one named last changes fastest.
Arguments:
- segment_launch_values: float32 [4, 3, 1024, 1024], P('sub', None, 'lat', 'lon'), may hold values from -1.8 to 1.8
- initial_backdrop: float32 [3, 1024, 1024], P(None, 'lat', 'lon'), may hold values from -1.8 to 1.8
- spectral_inverse_variances: float32 [3, 513], replicated, may hold values from 0.3 to 3
Outputs:
- weighted_defects: float32 [4, 3, 1024, 1024], P('sub', None, 'lat', 'lon')
The draws below stay inside these ranges and needn't reach their ends.
All inputs are finite; a program needn't handle non-finite values.
Results may differ from the reference program's by a relative error of at most 0.00017.
Values sent between devices are 32-bit elements; how exact they have to be, the bound alone decides.
A program may use at most 64 MiB of HBM per device.

```python
import math
import jax
import jax.numpy as jnp
from jax import lax

NLON = 1024
STEPS = 3
NLAT = 1024
NSUB = 4
ZONAL_MODES = 513


def level_of(own_key, dims, shards, least, high):
    def one(axis_at, shards_of):
        draws = jax.random.uniform(jax.random.fold_in(jax.random.fold_in(own_key, 6), axis_at), (shards_of,), jnp.float32, least / len(shards), high / len(shards))
        return jnp.repeat(jnp.exp(draws), dims[axis_at] // shards_of).reshape((-1,) + (1,) * (len(dims) - axis_at - 1))

    factor_of = one(*shards[0])
    for cut in shards[1:]:
        factor_of = factor_of * one(*cut)
    return factor_of


def centred(key, extent, width, limit, shards=(), dtype=jnp.bfloat16):
    values = width * jax.random.normal(key, extent, jnp.float32)
    if shards:
        values = values * level_of(key, extent, shards, -0.22, 0.18)
    return jnp.clip(values, -limit, limit).astype(dtype)


def setup_inputs(seed: int = 0) -> dict:
    key_of = jax.random.split(jax.random.key(seed), 4)
    return {
        "segment_launch_values": centred(key_of[0], (NSUB, 3, NLAT, NLON), 0.3, 1.8, ((0, 4), (2, 2), (3, 4)), jnp.float32),
        "initial_backdrop": centred(key_of[1], (3, NLAT, NLON), 0.3, 1.8, ((1, 2), (2, 4)), jnp.float32),
        "spectral_inverse_variances": jnp.clip(jnp.exp(jax.random.uniform(key_of[2], (3, ZONAL_MODES), jnp.float32, math.log(0.3), math.log(3.0))), 0.3, 3.0),
    }


time_step = 0.5
coriolis_peak = 0.4


def latitude_tendencies(total_rows, first_row, count):
    index = (first_row + jnp.arange(count)).astype(jnp.float32)
    return (coriolis_peak * jnp.sin(2.0 * jnp.pi * (index + 0.5) / total_rows))[:, None]


def centre(field):
    return field[1:-1, 1:-1]


def along_lon(field):
    return 0.5 * (field[1:-1, 2:] - field[1:-1, :-2])


def along_lat(field):
    return 0.5 * (field[2:, 1:-1] - field[:-2, 1:-1])


def tendency(padded, coriolis):
    height = padded[0]
    zonal = padded[1]
    meridional = padded[2]
    depth = 1.0 + height
    height_rate = -(along_lon(depth * zonal) + along_lat(depth * meridional))
    zonal_mid = centre(zonal)
    merid_mid = centre(meridional)
    zonal_rate = -(zonal_mid * along_lon(zonal) + merid_mid * along_lat(zonal)) + coriolis * merid_mid - along_lon(height)
    merid_rate = -(zonal_mid * along_lon(meridional) + merid_mid * along_lat(meridional)) - coriolis * zonal_mid - along_lat(height)
    return jnp.stack([height_rate, zonal_rate, merid_rate])


def wrapped_rate(flow_variables, coriolis):
    padded = jnp.pad(flow_variables, ((0, 0), (1, 1), (1, 1)), mode="wrap")
    return tendency(padded, coriolis)


def model_step(flow_variables, coriolis):
    first = flow_variables + time_step * wrapped_rate(flow_variables, coriolis)
    second = 0.75 * flow_variables + 0.25 * (first + time_step * wrapped_rate(first, coriolis))
    return (1.0 / 3.0) * flow_variables + (2.0 / 3.0) * (second + time_step * wrapped_rate(second, coriolis))


def reference(segment_launch_values, initial_backdrop, spectral_inverse_variances):
    coriolis = latitude_tendencies(NLAT, 0, NLAT)

    def propagated_estimate(flow_variables):
        for step_number in range(STEPS):
            flow_variables = model_step(flow_variables, coriolis)
        return flow_variables

    interval_predictions = lax.map(propagated_estimate, segment_launch_values)
    preceding_interval = jnp.concatenate([initial_backdrop[None], interval_predictions[:-1]], axis=0)
    mismatch_misfits = segment_launch_values - preceding_interval
    spectral_coefficients = jnp.fft.rfft(mismatch_misfits, axis=-1) * spectral_inverse_variances[None, :, None, :]
    return jnp.fft.irfft(spectral_coefficients, n=NLON, axis=-1).astype(jnp.float32)
```

```python
import numpy as np
import jax
import jax.numpy as jnp
from jax import lax
from jax.experimental import pallas as pl
from jax.experimental.pallas import tpu as pltpu
from jax.sharding import PartitionSpec as P

STEPS = 3
HALO = 16
BLOCK = 4
MESH = pl.DeviceIdType.MESH

time_step = 0.5
coriolis_peak = 0.4


def cosine_table(length):
    half = length // 2
    wave = np.arange(half)[:, None]
    angle = (wave * np.arange(length)[None, :]) % length * (2.0 * np.pi / length)
    return (np.where(wave == 0, 1.0, 2.0) / length * np.cos(angle)).astype(np.float32)


def doubled_coriolis(total_rows):
    index = np.arange(total_rows)
    return (2.0 * coriolis_peak * np.sin(2.0 * np.pi * (index + 0.5) / total_rows)).astype(
        np.float32
    )


def split_parts(value):
    high = value.astype(jnp.bfloat16)
    return high, (value - high.astype(jnp.float32)).astype(jnp.bfloat16)


def kernel(
    nsub, nlat, nlon, x_hbm, back_hbm, w_ref, table_hbm, f_smem, out_ref,
    table, wpad, wave_row, conv_hi, conv_lo, frows, slab, fc, state, mid1, mid2,
    y_own, y_next, got_own, got_next,
    table_sem, main_send, top_send, bot_send, main_recv, top_recv, bot_recv,
    back_send, back_recv, own_send, own_recv, next_send, next_recv,
):
    k = lax.axis_index("sub")
    a = lax.axis_index("lat")
    z = lax.axis_index("lon")
    fields, lat_rows, width = x_hbm.shape
    rows = lat_rows // nlon
    total = lat_rows * nlat
    length = width * nlon
    half = length // 2
    lanes = 128
    slices = length // lanes
    padded = rows + 2 * HALO
    k_up = lax.rem(k + 1, nsub)
    k_down = lax.rem(k + nsub - 1, nsub)
    a_up = lax.rem(a + 1, nlat)
    a_down = lax.rem(a + nlat - 1, nlat)
    last = nsub - 1

    barrier = pltpu.get_barrier_semaphore()
    for d in range(1, nlon):
        pl.semaphore_signal(
            barrier, inc=1, device_id=(k, a, lax.rem(z + d, nlon)), device_id_type=MESH
        )
    for d in range(nlon):
        for there in ((k, a_up), (k, a_down), (k_up, a), (k_down, a)):
            pl.semaphore_signal(barrier, inc=1, device_id=there + (jnp.int32(d),), device_id_type=MESH)
    pl.semaphore_wait(barrier, nlon - 1 + 4 * nlon)

    mine = pl.ds(pl.multiple_of(z * width, width), width)

    def local(src, dst, sem):
        return pltpu.make_async_copy(src, dst, sem)

    def remote(src, dst, send, recv, there):
        return pltpu.make_async_remote_copy(
            src_ref=src, dst_ref=dst, send_sem=send, recv_sem=recv,
            device_id=there, device_id_type=MESH,
        )

    def rows_at(first, count):
        return pl.ds(pl.multiple_of(first, 8), count)

    def edge(target, up):
        if up:
            src = x_hbm.at[:, pl.ds(target * rows + rows - HALO, HALO), :]
            dst = slab.at[:, pl.ds(0, HALO), mine]
            lon, lat = (target + 1) % nlon, a_up if target == nlon - 1 else a
            send, recv = top_send.at[target], top_recv.at[z]
        else:
            src = x_hbm.at[:, pl.ds(target * rows, HALO), :]
            dst = slab.at[:, pl.ds(HALO + rows, HALO), mine]
            lon, lat = (target - 1) % nlon, a_down if target == 0 else a
            send, recv = bot_send.at[target], bot_recv.at[z]
        crosses = target == (nlon - 1 if up else 0)
        return src, dst, send, recv, lon, lat, crosses

    def exchange(src_hbm, dst, sends, recvs, first):
        def copy_of(d):
            zt = lax.rem(z + d, nlon)
            src = src_hbm.at[:, rows_at(zt * rows, rows), :]
            into = dst.at[:, pl.ds(first, rows), mine]
            if d == 0:
                return local(src, into, recvs.at[z])
            return remote(src, into, sends.at[d], recvs.at[z], (k, a, zt))

        return [copy_of(d) for d in range(nlon)]

    mains = exchange(x_hbm, slab, main_send, main_recv, HALO)
    for d in (1, nlon - 1) if nlon > 2 else (1,):
        mains[d].start()
    for d in range(2, nlon - 1):
        mains[d].start()
    mains[0].start()
    for up in (True, False):
        for target in range(nlon):
            src, dst, send, recv, lon, lat, crosses = edge(target, up)
            if crosses:
                remote(src, dst, send, recv, (k, lat, jnp.int32(lon))).start()
            else:
                @pl.when(z == lon)
                def _():
                    local(src, dst, recv).start()

                @pl.when(z != lon)
                def _():
                    remote(src, dst, send, recv, (k, lat, jnp.int32(lon))).start()

    table_copy = local(table_hbm, table, table_sem)
    table_copy.start()
    wpad[...] = jnp.zeros_like(wpad)
    wpad[0:fields, 0 : half + 1] = w_ref[...]
    table_copy.wait()
    sign = 1.0 - 2.0 * (lax.broadcasted_iota(jnp.int32, (8, length), 1) % 2).astype(jnp.float32)
    wave_row[...] = (
        jnp.dot(
            wpad[:, 0:half], table[...], precision=lax.Precision.HIGHEST,
            preferred_element_type=jnp.float32,
        )
        + wpad[:, half : half + 1] * (sign / length)
    )
    chunk = 16
    blocks = half // lanes
    for c in range(fields):
        line = 0.5 * wave_row[c : c + 1, :]

        @pl.loop(0, lanes // chunk)
        def _(i):
            row = i * chunk + lax.broadcasted_iota(jnp.int32, (chunk, length), 0)
            turned = jnp.broadcast_to(line, (chunk, length))
            for bit in range(lanes.bit_length() - 1):
                far = pltpu.roll(turned, 1 << bit, 1)
                turned = jnp.where((row >> bit) % 2 == 1, far, turned)
            for q in range(slices):
                first = turned[:, q * lanes : (q + 1) * lanes]
                p = (q + blocks) % slices
                other = turned[:, p * lanes : (p + 1) * lanes]
                for part, value in enumerate((first + other, first - other)):
                    high, low = split_parts(value)
                    for m in range(blocks):
                        t = (q + m) % slices
                        if t < blocks:
                            at = pl.ds(pl.multiple_of(m * lanes + i * chunk, chunk), chunk)
                            conv_hi[2 * c + part, at, t * lanes : (t + 1) * lanes] = high
                            conv_lo[2 * c + part, at, t * lanes : (t + 1) * lanes] = low

    first_row = (a * nlon + z) * rows - HALO + total

    @pl.loop(0, padded)
    def _(r):
        frows[pl.ds(pl.multiple_of(8 * r, 8), 8), :] = jnp.full(
            (8, lanes), f_smem[lax.rem(first_row + r, total)], jnp.float32
        )

    for s in range(nlon):
        cols = pl.ds(s * width, width)
        for first, count, recv in (
            (HALO, rows, main_recv), (0, HALO, top_recv), (HALO + rows, HALO, bot_recv)
        ):
            block = slab.at[:, pl.ds(first, count), cols]
            local(block, block, recv.at[s]).wait()

    backs = exchange(back_hbm, fc, back_send, back_recv, 0)

    @pl.when(k == last)
    def _():
        for d in range(nlon):
            backs[d].start()

    def filtered(source, first, c):
        value = source[c, pl.ds(first, rows), :]
        left, right = value[:, :half], value[:, half:]
        halves = []
        for part, mix in enumerate((left + right, left - right)):
            high, low = split_parts(mix)
            both = jnp.concatenate([high, low], axis=0)
            twice = jnp.dot(both, conv_hi[2 * c + part], preferred_element_type=jnp.float32)
            rest = jnp.dot(high, conv_lo[2 * c + part], preferred_element_type=jnp.float32)
            halves.append(twice[:rows] + (twice[rows:] + rest))
        return halves[0] + halves[1], halves[0] - halves[1]

    def home(c, d, y, got, sends, recvs, sub, own):
        zt = lax.rem(z + d, nlon)
        src = y.at[c, :, pl.ds(pl.multiple_of(zt * width, width), width)]
        dst = got.at[c, rows_at(z * rows, rows), :]
        if own and d == 0:
            return local(src, dst, recvs.at[c, z])
        return remote(src, dst, sends.at[c, d], recvs.at[c, z], (sub, a, zt))

    order = [d for d in (1, nlon - 1) if d > 0]
    order = list(dict.fromkeys(order)) + [d for d in range(2, nlon - 1)] + [0]

    def filter_and_send(source, first, y, got, sends, recvs, sub, own):
        @pl.loop(0, fields)
        def _(c):
            low, high = filtered(source, first, c)
            y[c, :, 0:half] = low
            y[c, :, half:length] = high
            for d in order:
                home(c, d, y, got, sends, recvs, sub, own).start()

    filter_and_send(slab, HALO, y_own, got_own, own_send, own_recv, k, True)

    @pl.when(k < last)
    def _():
        group = 32

        @pl.loop(0, padded // group)
        def _(i):
            r0 = pl.multiple_of(i * group, group)
            for c in range(fields):
                for s in range(slices):
                    state[c, pl.ds(8 * r0 + s, group, stride=8), :] = slab[
                        c, pl.ds(r0, group), s * lanes : (s + 1) * lanes
                    ]

        lane = lax.broadcasted_iota(jnp.int32, (BLOCK, 8, lanes), 2)
        at_first, at_last = lane == 0, lane == lanes - 1

        def across(v):
            ahead = pltpu.roll(jnp.where(at_first, pltpu.roll(v, 7, 1), v), lanes - 1, 2)
            behind = pltpu.roll(jnp.where(at_last, pltpu.roll(v, 1, 1), v), 1, 2)
            return ahead - behind

        def stage(arg, base, out, keep, mix, gain):
            @pl.loop(0, (padded - HALO) // BLOCK)
            def _(i):
                r0 = 8 + i * BLOCK
                wide = pl.ds(pl.multiple_of(8 * (r0 - 1), 8), 8 * (BLOCK + 2))
                at = pl.ds(pl.multiple_of(8 * r0, 8), 8 * BLOCK)
                h, u, v = [arg[c, wide, :].reshape(BLOCK + 2, 8, lanes) for c in range(3)]
                f2 = frows[at, :].reshape(BLOCK, 8, lanes)
                hm, um, vm = [q[1:-1] for q in (h, u, v)]

                def along(q):
                    return q[2:] - q[:-2]

                dv = v + h * v
                rate_h = across(um + hm * um) + along(dv)
                rate_u = um * across(um) + vm * along(u) + across(hm) - f2 * vm
                rate_v = um * across(vm) + vm * along(v) + along(h) + f2 * um
                for c, (m, rate) in enumerate(((hm, rate_h), (um, rate_u), (vm, rate_v))):
                    if base is None:
                        value = m - gain * rate
                    else:
                        old = base[c, at, :].reshape(BLOCK, 8, lanes)
                        value = keep * old + mix * m - gain * rate
                    out[c, at, :] = value.reshape(8 * BLOCK, lanes)

        half_step = 0.5 * time_step

        @pl.loop(0, STEPS)
        def _(step):
            stage(state, None, mid1, 0.0, 1.0, half_step)
            stage(mid1, state, mid2, 0.75, 0.25, 0.25 * half_step)
            stage(mid2, state, state, 1.0 / 3.0, 2.0 / 3.0, 2.0 / 3.0 * half_step)

        @pl.loop(0, rows // group)
        def _(i):
            r0 = pl.multiple_of(i * group, group)
            for c in range(fields):
                for s in range(slices):
                    fc[c, pl.ds(r0, group), s * lanes : (s + 1) * lanes] = state[
                        c, pl.ds(8 * (r0 + HALO) + s, group, stride=8), :
                    ]

    @pl.when(k == last)
    def _():
        for s in range(nlon):
            block = fc.at[:, :, pl.ds(s * width, width)]
            local(block, block, back_recv.at[s]).wait()
        for d in range(1, nlon):
            backs[d].wait_send()

    filter_and_send(fc, 0, y_next, got_next, next_send, next_recv, k_up, False)

    for c in range(fields):
        for s in range(nlon):
            for got, recvs in ((got_own, own_recv), (got_next, next_recv)):
                block = got.at[c, pl.ds(s * rows, rows), :]
                local(block, block, recvs.at[c, s]).wait()
            part = pl.ds(s * rows, rows)
            out_ref[c, part, :] = got_own[c, part, :] - got_next[c, part, :]

    for d in range(1, nlon):
        mains[d].wait_send()
    for up in (True, False):
        for target in range(nlon):
            src, dst, send, recv, lon, lat, crosses = edge(target, up)
            if crosses:
                remote(src, dst, send, recv, (k, lat, jnp.int32(lon))).wait_send()
            else:
                @pl.when(z != lon)
                def _():
                    remote(src, dst, send, recv, (k, lat, jnp.int32(lon))).wait_send()
    for c in range(fields):
        for d in range(nlon):
            if d:
                home(c, d, y_own, got_own, own_send, own_recv, k, True).wait_send()
            home(c, d, y_next, got_next, next_send, next_recv, k_up, False).wait_send()


def solution(mesh):
    nsub, nlat, nlon = mesh.shape["sub"], mesh.shape["lat"], mesh.shape["lon"]

    def shards(launch, backdrop, inverse_variances):
        tile = launch[0]
        fields, lat_rows, width = tile.shape
        length = width * nlon
        half = length // 2
        rows = lat_rows // nlon
        padded = rows + 2 * HALO
        f32, bf16 = jnp.float32, jnp.bfloat16
        dma = pltpu.SemaphoreType.DMA
        any_space = pl.BlockSpec(memory_space=pl.ANY)
        vmem = pl.BlockSpec(memory_space=pltpu.VMEM)
        rows_like = pltpu.VMEM((fields, padded * 8, 128), f32)
        tile_like = pltpu.VMEM((fields, lat_rows, width), f32)
        slab_like = pltpu.VMEM((fields, rows, length), f32)
        out = pl.pallas_call(
            lambda *refs: kernel(nsub, nlat, nlon, *refs),
            name="weighted_defects",
            out_shape=jax.ShapeDtypeStruct(tile.shape, f32),
            in_specs=[any_space, any_space, vmem, any_space,
                      pl.BlockSpec(memory_space=pltpu.SMEM)],
            out_specs=vmem,
            scratch_shapes=[
                pltpu.VMEM((half, length), f32),
                pltpu.VMEM((8, half + 128), f32),
                pltpu.VMEM((8, length), f32),
                pltpu.VMEM((2 * fields, half, half), bf16),
                pltpu.VMEM((2 * fields, half, half), bf16),
                pltpu.VMEM((padded * 8, 128), f32),
                pltpu.VMEM((fields, padded, length), f32),
                slab_like,
                rows_like, rows_like, rows_like,
                slab_like, slab_like, tile_like, tile_like,
                dma,
                dma((nlon,)), dma((nlon,)), dma((nlon,)),
                dma((nlon,)), dma((nlon,)), dma((nlon,)),
                dma((nlon,)), dma((nlon,)),
                dma((fields, nlon)), dma((fields, nlon)),
                dma((fields, nlon)), dma((fields, nlon)),
            ],
            compiler_params=pltpu.CompilerParams(collective_id=0, has_side_effects=True),
        )(
            tile, backdrop, inverse_variances,
            jnp.asarray(cosine_table(length)), jnp.asarray(doubled_coriolis(lat_rows * nlat)),
        )
        return out[None]

    return jax.shard_map(
        shards,
        mesh=mesh,
        in_specs=(P("sub", None, "lat", "lon"), P(None, "lat", "lon"), P()),
        out_specs=P("sub", None, "lat", "lon"),
        check_vma=False,
    )
```

```python
import numpy as np
import jax
import jax.numpy as jnp
from jax import lax
from jax.experimental import pallas as pl
from jax.experimental.pallas import tpu as pltpu
from jax.sharding import PartitionSpec as P

STEPS = 3
HALO = 16
BLOCK = 4
MESH = pl.DeviceIdType.MESH

time_step = 0.5
coriolis_peak = 0.4


def cosine_table(length):
    half = length // 2
    wave = np.arange(half)[:, None]
    angle = (wave * np.arange(length)[None, :]) % length * (2.0 * np.pi / length)
    return (np.where(wave == 0, 1.0, 2.0) / length * np.cos(angle)).astype(np.float32)


def doubled_coriolis(total_rows):
    index = np.arange(total_rows)
    return (2.0 * coriolis_peak * np.sin(2.0 * np.pi * (index + 0.5) / total_rows)).astype(
        np.float32
    )


def split_parts(value):
    high = value.astype(jnp.bfloat16)
    return high, (value - high.astype(jnp.float32)).astype(jnp.bfloat16)


def kernel(
    nsub, nlat, nlon, x_hbm, back_hbm, w_ref, table_hbm, f_smem, out_ref,
    table, wpad, wave_row, conv_hi, conv_lo, frows, slab, fc, state, mid1, mid2,
    prev, y_own, got_own,
    table_sem, main_send, top_send, bot_send, main_recv, top_recv, bot_recv,
    back_send, back_recv, own_send, own_recv, hop_send, hop_recv,
):
    k = lax.axis_index("sub")
    a = lax.axis_index("lat")
    z = lax.axis_index("lon")
    fields, lat_rows, width = x_hbm.shape
    rows = lat_rows // nlon
    total = lat_rows * nlat
    length = width * nlon
    half = length // 2
    lanes = 128
    slices = length // lanes
    padded = rows + 2 * HALO
    k_up = lax.rem(k + 1, nsub)
    k_down = lax.rem(k + nsub - 1, nsub)
    a_up = lax.rem(a + 1, nlat)
    a_down = lax.rem(a + nlat - 1, nlat)
    last = nsub - 1

    barrier = pltpu.get_barrier_semaphore()
    for d in range(1, nlon):
        pl.semaphore_signal(
            barrier, inc=1, device_id=(k, a, lax.rem(z + d, nlon)), device_id_type=MESH
        )
    for d in range(nlon):
        for there in ((k, a_up), (k, a_down), (k_up, a), (k_down, a)):
            pl.semaphore_signal(barrier, inc=1, device_id=there + (jnp.int32(d),), device_id_type=MESH)
    pl.semaphore_wait(barrier, nlon - 1 + 4 * nlon)

    mine = pl.ds(pl.multiple_of(z * width, width), width)

    def local(src, dst, sem):
        return pltpu.make_async_copy(src, dst, sem)

    def remote(src, dst, send, recv, there):
        return pltpu.make_async_remote_copy(
            src_ref=src, dst_ref=dst, send_sem=send, recv_sem=recv,
            device_id=there, device_id_type=MESH,
        )

    def rows_at(first, count):
        return pl.ds(pl.multiple_of(first, 8), count)

    def edge(target, up):
        if up:
            src = x_hbm.at[:, pl.ds(target * rows + rows - HALO, HALO), :]
            dst = slab.at[:, pl.ds(0, HALO), mine]
            lon, lat = (target + 1) % nlon, a_up if target == nlon - 1 else a
            send, recv = top_send.at[target], top_recv.at[z]
        else:
            src = x_hbm.at[:, pl.ds(target * rows, HALO), :]
            dst = slab.at[:, pl.ds(HALO + rows, HALO), mine]
            lon, lat = (target - 1) % nlon, a_down if target == 0 else a
            send, recv = bot_send.at[target], bot_recv.at[z]
        crosses = target == (nlon - 1 if up else 0)
        return src, dst, send, recv, lon, lat, crosses

    def exchange(src_hbm, dst, sends, recvs, first):
        def copy_of(d):
            zt = lax.rem(z + d, nlon)
            src = src_hbm.at[:, rows_at(zt * rows, rows), :]
            into = dst.at[:, pl.ds(first, rows), mine]
            if d == 0:
                return local(src, into, recvs.at[z])
            return remote(src, into, sends.at[d], recvs.at[z], (k, a, zt))

        return [copy_of(d) for d in range(nlon)]

    mains = exchange(x_hbm, slab, main_send, main_recv, HALO)
    for d in (1, nlon - 1) if nlon > 2 else (1,):
        mains[d].start()
    for d in range(2, nlon - 1):
        mains[d].start()
    mains[0].start()
    for up in (True, False):
        for target in range(nlon):
            src, dst, send, recv, lon, lat, crosses = edge(target, up)
            if crosses:
                remote(src, dst, send, recv, (k, lat, jnp.int32(lon))).start()
            else:
                @pl.when(z == lon)
                def _():
                    local(src, dst, recv).start()

                @pl.when(z != lon)
                def _():
                    remote(src, dst, send, recv, (k, lat, jnp.int32(lon))).start()

    table_copy = local(table_hbm, table, table_sem)
    table_copy.start()
    wpad[...] = jnp.zeros_like(wpad)
    wpad[0:fields, 0 : half + 1] = w_ref[...]
    table_copy.wait()
    sign = 1.0 - 2.0 * (lax.broadcasted_iota(jnp.int32, (8, length), 1) % 2).astype(jnp.float32)
    wave_row[...] = (
        jnp.dot(
            wpad[:, 0:half], table[...], precision=lax.Precision.HIGHEST,
            preferred_element_type=jnp.float32,
        )
        + wpad[:, half : half + 1] * (sign / length)
    )
    chunk = 16
    blocks = half // lanes
    for c in range(fields):
        line = 0.5 * wave_row[c : c + 1, :]

        @pl.loop(0, lanes // chunk)
        def _(i):
            row = i * chunk + lax.broadcasted_iota(jnp.int32, (chunk, length), 0)
            turned = jnp.broadcast_to(line, (chunk, length))
            for bit in range(lanes.bit_length() - 1):
                far = pltpu.roll(turned, 1 << bit, 1)
                turned = jnp.where((row >> bit) % 2 == 1, far, turned)
            for q in range(slices):
                first = turned[:, q * lanes : (q + 1) * lanes]
                p = (q + blocks) % slices
                other = turned[:, p * lanes : (p + 1) * lanes]
                for part, value in enumerate((first + other, first - other)):
                    high, low = split_parts(value)
                    for m in range(blocks):
                        t = (q + m) % slices
                        if t < blocks:
                            at = pl.ds(pl.multiple_of(m * lanes + i * chunk, chunk), chunk)
                            conv_hi[2 * c + part, at, t * lanes : (t + 1) * lanes] = high
                            conv_lo[2 * c + part, at, t * lanes : (t + 1) * lanes] = low

    first_row = (a * nlon + z) * rows - HALO + total

    @pl.loop(0, padded)
    def _(r):
        frows[pl.ds(pl.multiple_of(8 * r, 8), 8), :] = jnp.full(
            (8, lanes), f_smem[lax.rem(first_row + r, total)], jnp.float32
        )

    for s in range(nlon):
        cols = pl.ds(s * width, width)
        for first, count, recv in (
            (HALO, rows, main_recv), (0, HALO, top_recv), (HALO + rows, HALO, bot_recv)
        ):
            block = slab.at[:, pl.ds(first, count), cols]
            local(block, block, recv.at[s]).wait()

    backs = exchange(back_hbm, fc, back_send, back_recv, 0)

    @pl.when(k == last)
    def _():
        for d in range(nlon):
            backs[d].start()

    def filtered(c):
        value = slab[c, pl.ds(HALO, rows), :] - prev[c]
        left, right = value[:, :half], value[:, half:]
        halves = []
        for part, mix in enumerate((left + right, left - right)):
            high, low = split_parts(mix)
            both = jnp.concatenate([high, low], axis=0)
            twice = jnp.dot(both, conv_hi[2 * c + part], preferred_element_type=jnp.float32)
            rest = jnp.dot(high, conv_lo[2 * c + part], preferred_element_type=jnp.float32)
            halves.append(twice[:rows] + (twice[rows:] + rest))
        return halves[0] + halves[1], halves[0] - halves[1]

    def home(c, d):
        zt = lax.rem(z + d, nlon)
        src = y_own.at[c, :, pl.ds(pl.multiple_of(zt * width, width), width)]
        dst = got_own.at[c, rows_at(z * rows, rows), :]
        if d == 0:
            return local(src, dst, own_recv.at[c, z])
        return remote(src, dst, own_send.at[c, d], own_recv.at[c, z], (k, a, zt))

    def hop(c):
        return remote(fc.at[c], prev.at[c], hop_send.at[c], hop_recv.at[c], (k_up, a, z))

    order = [d for d in (1, nlon - 1) if d > 0]
    order = list(dict.fromkeys(order)) + [d for d in range(2, nlon - 1)] + [0]

    @pl.when(k < last)
    def _():
        group = 32

        @pl.loop(0, padded // group)
        def _(i):
            r0 = pl.multiple_of(i * group, group)
            for c in range(fields):
                for s in range(slices):
                    state[c, pl.ds(8 * r0 + s, group, stride=8), :] = slab[
                        c, pl.ds(r0, group), s * lanes : (s + 1) * lanes
                    ]

        lane = lax.broadcasted_iota(jnp.int32, (BLOCK, 8, lanes), 2)
        at_first, at_last = lane == 0, lane == lanes - 1

        def across(v):
            ahead = pltpu.roll(jnp.where(at_first, pltpu.roll(v, 7, 1), v), lanes - 1, 2)
            behind = pltpu.roll(jnp.where(at_last, pltpu.roll(v, 1, 1), v), 1, 2)
            return ahead - behind

        def stage(arg, base, out, keep, mix, gain):
            @pl.loop(0, (padded - HALO) // BLOCK)
            def _(i):
                r0 = 8 + i * BLOCK
                wide = pl.ds(pl.multiple_of(8 * (r0 - 1), 8), 8 * (BLOCK + 2))
                at = pl.ds(pl.multiple_of(8 * r0, 8), 8 * BLOCK)
                h, u, v = [arg[c, wide, :].reshape(BLOCK + 2, 8, lanes) for c in range(3)]
                f2 = frows[at, :].reshape(BLOCK, 8, lanes)
                hm, um, vm = [q[1:-1] for q in (h, u, v)]

                def along(q):
                    return q[2:] - q[:-2]

                dv = v + h * v
                rate_h = across(um + hm * um) + along(dv)
                rate_u = um * across(um) + vm * along(u) + across(hm) - f2 * vm
                rate_v = um * across(vm) + vm * along(v) + along(h) + f2 * um
                for c, (m, rate) in enumerate(((hm, rate_h), (um, rate_u), (vm, rate_v))):
                    if base is None:
                        value = m - gain * rate
                    else:
                        old = base[c, at, :].reshape(BLOCK, 8, lanes)
                        value = keep * old + mix * m - gain * rate
                    out[c, at, :] = value.reshape(8 * BLOCK, lanes)

        half_step = 0.5 * time_step

        @pl.loop(0, STEPS)
        def _(step):
            stage(state, None, mid1, 0.0, 1.0, half_step)
            stage(mid1, state, mid2, 0.75, 0.25, 0.25 * half_step)
            stage(mid2, state, state, 1.0 / 3.0, 2.0 / 3.0, 2.0 / 3.0 * half_step)

        @pl.loop(0, rows // group)
        def _(i):
            r0 = pl.multiple_of(i * group, group)
            for c in range(fields):
                for s in range(slices):
                    fc[c, pl.ds(r0, group), s * lanes : (s + 1) * lanes] = state[
                        c, pl.ds(8 * (r0 + HALO) + s, group, stride=8), :
                    ]

    @pl.when(k == last)
    def _():
        for s in range(nlon):
            block = fc.at[:, :, pl.ds(s * width, width)]
            local(block, block, back_recv.at[s]).wait()
        for d in range(1, nlon):
            backs[d].wait_send()

    for c in range(fields):
        hop(c).start()

    @pl.loop(0, fields)
    def _(c):
        hop(c).wait_recv()
        low, high = filtered(c)
        y_own[c, :, 0:half] = low
        y_own[c, :, half:length] = high
        for d in order:
            home(c, d).start()

    for c in range(fields):
        for s in range(nlon):
            part = pl.ds(s * rows, rows)
            block = got_own.at[c, part, :]
            local(block, block, own_recv.at[c, s]).wait()
            out_ref[c, part, :] = got_own[c, part, :]

    for d in range(1, nlon):
        mains[d].wait_send()
    for up in (True, False):
        for target in range(nlon):
            src, dst, send, recv, lon, lat, crosses = edge(target, up)
            if crosses:
                remote(src, dst, send, recv, (k, lat, jnp.int32(lon))).wait_send()
            else:
                @pl.when(z != lon)
                def _():
                    remote(src, dst, send, recv, (k, lat, jnp.int32(lon))).wait_send()
    for c in range(fields):
        for d in range(nlon):
            if d:
                home(c, d).wait_send()
        hop(c).wait_send()


def solution(mesh):
    nsub, nlat, nlon = mesh.shape["sub"], mesh.shape["lat"], mesh.shape["lon"]

    def shards(launch, backdrop, inverse_variances):
        tile = launch[0]
        fields, lat_rows, width = tile.shape
        length = width * nlon
        half = length // 2
        rows = lat_rows // nlon
        padded = rows + 2 * HALO
        f32, bf16 = jnp.float32, jnp.bfloat16
        dma = pltpu.SemaphoreType.DMA
        any_space = pl.BlockSpec(memory_space=pl.ANY)
        vmem = pl.BlockSpec(memory_space=pltpu.VMEM)
        rows_like = pltpu.VMEM((fields, padded * 8, 128), f32)
        tile_like = pltpu.VMEM((fields, lat_rows, width), f32)
        slab_like = pltpu.VMEM((fields, rows, length), f32)
        out = pl.pallas_call(
            lambda *refs: kernel(nsub, nlat, nlon, *refs),
            name="weighted_defects",
            out_shape=jax.ShapeDtypeStruct(tile.shape, f32),
            in_specs=[any_space, any_space, vmem, any_space,
                      pl.BlockSpec(memory_space=pltpu.SMEM)],
            out_specs=vmem,
            scratch_shapes=[
                pltpu.VMEM((half, length), f32),
                pltpu.VMEM((8, half + 128), f32),
                pltpu.VMEM((8, length), f32),
                pltpu.VMEM((2 * fields, half, half), bf16),
                pltpu.VMEM((2 * fields, half, half), bf16),
                pltpu.VMEM((padded * 8, 128), f32),
                pltpu.VMEM((fields, padded, length), f32),
                slab_like,
                rows_like, rows_like, rows_like,
                slab_like, slab_like, tile_like,
                dma,
                dma((nlon,)), dma((nlon,)), dma((nlon,)),
                dma((nlon,)), dma((nlon,)), dma((nlon,)),
                dma((nlon,)), dma((nlon,)),
                dma((fields, nlon)), dma((fields, nlon)),
                dma((fields,)), dma((fields,)),
            ],
            compiler_params=pltpu.CompilerParams(collective_id=0, has_side_effects=True),
        )(
            tile, backdrop, inverse_variances,
            jnp.asarray(cosine_table(length)), jnp.asarray(doubled_coriolis(lat_rows * nlat)),
        )
        return out[None]

    return jax.shard_map(
        shards,
        mesh=mesh,
        in_specs=(P("sub", None, "lat", "lon"), P(None, "lat", "lon"), P()),
        out_specs=P("sub", None, "lat", "lon"),
        check_vma=False,
    )
```
